256 devices in a mesh: cfg: 2 (over z), tm: 16 (over x, core), space: 8 (over y).
Axes of the slice: x: 8, y: 8, z: 2, core: 2. Of those that a mesh axis runs over, the one named last changes fastest.
The devices are a block of a 8x8x16 slice.
Arguments:
- solutions: bfloat16 [32, 2, 3, 1024, 384], P(('cfg', 'tm'), None, None, 'space'), parts along dimension 0, may hold values from -6 to 6
- eigvecs: bfloat16 [32, 2, 3, 1024, 384], P(('cfg', 'tm'), None, None, 'space'), parts along dimension 0, may hold values from -0.078125 to 0.078125
- meson: bfloat16 [4, 32, 2, 384, 384], P(None, ('cfg', 'tm')), parts along dimension 1, may hold values from -0.015625 to 0.015625
- momenta: int32 [4, 3], replicated, may hold values from -3 to 3
- source_time: int32 [384], replicated, may hold values from 0 to 15
- dilution: int32 [384], replicated, may hold values from 0 to 3
Outputs:
- blocks: float32 [4, 2, 384, 32, 384], P(None, None, ('tm', 'space'), 'cfg'), parts along dimension 3
The draws below stay inside these ranges and needn't reach their ends.
There are 2 independent parts, one for each index of `cfg`. The reference program is written for one: setup_inputs(seed, part) draws one part's arguments, and reference() takes and returns one part's arrays. A program takes and returns all parts, laid end to end along the dimension named above; an argument that names none is the same for every part. Nothing has to cross between parts.
All inputs are finite; a program needn't handle non-finite values.
Results may differ from the reference program's by a relative error of at most 0.0056.
Values may be sent and summed in bfloat16 or wider, within the bound.
No kernel may reach another device: no remote copies, remote signals or barrier semaphores. Data moves between devices by JAX's collectives and lax.ppermute only.
A program may use at most 64 MiB of HBM per device.

```python
import jax
import jax.numpy as jnp
from jax import lax

SIDE = 48
NEV = 384
NCOL = 384
MOMENTA = 4
NDIL = 4
XS = 1024
NT = 16


def plant(result, stream_key, smallest, high):
    spot = [jax.random.randint(jax.random.fold_in(stream_key, axis), (), 0, length) for axis, length in enumerate(result.shape)]
    longest = result.shape.index(max(result.shape))
    beside = spot[:longest] + [(spot[longest] + 1) % result.shape[longest]] + spot[longest + 1:]
    return result.at[tuple(spot)].set(smallest).at[tuple(beside)].set(high)


def shard_levels(own_key, shape, split, smallest, top_value):
    def one(axis_at, blocks):
        draws = jax.random.uniform(jax.random.fold_in(jax.random.fold_in(own_key, 6), axis_at), (blocks,), jnp.float32, smallest / len(split), top_value / len(split))
        return jnp.repeat(jnp.exp(draws), shape[axis_at] // blocks).reshape((-1,) + (1,) * (len(shape) - axis_at - 1))

    gain = one(*split[0])
    for cut in split[1:]:
        gain = gain * one(*cut)
    return gain


def bell_draw(key, extent, width, most, shards=(), held_as=jnp.bfloat16):
    level = shard_levels(key, extent, shards, -0.22, 0.18) if shards else 1.0
    array = jax.random.normal(key, extent, jnp.float32) * width * level
    return jnp.minimum(jnp.maximum(array, -most), most).astype(held_as)


def setup_inputs(seed: int = 0, part: int = 0) -> dict:
    key_of = jax.random.split(jax.random.key(seed), 7)
    part_splits = jax.random.split(jax.random.fold_in(key_of[6], part), 7)
    return {
        "solutions": bell_draw(part_splits[0], (NT, 2, 3, XS, NCOL), 1.0, 6.0, ((0, 16), (3, 8))),
        "eigvecs": bell_draw(part_splits[1], (NT, 2, 3, XS, NEV), (6 * XS) ** -0.5, 0.078125, ((0, 16), (3, 8))),
        "meson": bell_draw(part_splits[2], (MOMENTA, NT, 2, NEV, NEV), (NEV * NEV) ** -0.5, 0.015625, ((1, 16),)),
        "momenta": plant(jax.random.randint(key_of[3], (MOMENTA, 3), -3, 4), jax.random.fold_in(key_of[3], 1), -3, 3).astype(jnp.int32),
        "source_time": plant(jax.random.randint(key_of[4], (NCOL,), 0, NT), jax.random.fold_in(key_of[4], 1), 0, NT - 1).astype(jnp.int32),
        "dilution": plant(jax.random.randint(key_of[5], (NCOL,), 0, NDIL), jax.random.fold_in(key_of[5], 1), 0, NDIL - 1).astype(jnp.int32),
    }


def contract(first_op, second_op):
    return lax.dot_general(first_op, second_op, (((0,), (0,)), ((), ())), preferred_element_type=jnp.float32)


def reference(solutions, eigvecs, meson, momenta, source_time, dilution):
    site_index = jnp.arange(XS, dtype=jnp.int32)
    coordinates = jnp.stack([site_index % SIDE, (site_index // SIDE) % SIDE, site_index // (SIDE * SIDE)], 0)
    windings = jnp.sum(momenta[:, :, None] * coordinates[None], 1)
    angles = (2.0 * jnp.pi / SIDE) * windings.astype(jnp.float32)
    cosine = jnp.cos(angles)[:, None, :, None]
    sine_part = jnp.sin(angles)[:, None, :, None]

    def project(inputs):
        solution, vectors = inputs
        solve_real = solution[0].astype(jnp.float32)
        solve_imag = solution[1].astype(jnp.float32)
        phased_real = cosine * solve_real[None] + sine_part * solve_imag[None]
        phased_imag = cosine * solve_imag[None] - sine_part * solve_real[None]
        phased_real = jnp.moveaxis(phased_real, 0, -1).reshape(3 * XS, NCOL * MOMENTA).astype(jnp.bfloat16)
        phased_imag = jnp.moveaxis(phased_imag, 0, -1).reshape(3 * XS, NCOL * MOMENTA).astype(jnp.bfloat16)
        base_real = solution[0].reshape(3 * XS, NCOL)
        base_imag = solution[1].reshape(3 * XS, NCOL)
        vec_real = vectors[0].reshape(3 * XS, NEV)
        vec_imag = vectors[1].reshape(3 * XS, NEV)
        zero_real = contract(base_real, vec_real) + contract(base_imag, vec_imag)
        zero_imag = contract(base_imag, vec_real) - contract(base_real, vec_imag)
        mom_real = contract(phased_real, vec_real) + contract(phased_imag, vec_imag)
        mom_imag = contract(phased_imag, vec_real) - contract(phased_real, vec_imag)
        zero_mom = jnp.stack([zero_real, zero_imag], 1)[:, None]
        momentum = jnp.stack([mom_real, mom_imag], 1).reshape(NCOL, MOMENTA, 2, NEV)
        return jnp.concatenate([zero_mom, momentum], 1)

    coefficients = lax.map(project, (solutions, eigvecs)).astype(jnp.bfloat16)
    dilution_mask = ((jnp.arange(NEV, dtype=jnp.int32) % NDIL)[None, :] == dilution[:, None]).astype(jnp.bfloat16)
    zero_mom = coefficients[:, :, 0] * dilution_mask[None, :, None, :]
    momentum = coefficients[:, :, 1:]
    meson_real = meson[:, :, 0].astype(jnp.float32)
    meson_imag = meson[:, :, 1].astype(jnp.float32)
    coef_real = momentum[:, :, :, 0].astype(jnp.float32)
    coef_imag = momentum[:, :, :, 1].astype(jnp.float32)
    left_real = (jnp.einsum('tapk,ptkl->ptal', coef_real, meson_real) + jnp.einsum('tapk,ptkl->ptal', coef_imag, meson_imag)).astype(jnp.bfloat16).astype(jnp.float32)
    left_imag = (jnp.einsum('tapk,ptkl->ptal', coef_real, meson_imag) - jnp.einsum('tapk,ptkl->ptal', coef_imag, meson_real)).astype(jnp.bfloat16).astype(jnp.float32)
    zero_real = zero_mom[:, :, 0].astype(jnp.float32)
    zero_imag = zero_mom[:, :, 1].astype(jnp.float32)
    pair_real = jnp.einsum('ptal,tbl->ptab', left_real, zero_real) - jnp.einsum('ptal,tbl->ptab', left_imag, zero_imag)
    pair_imag = jnp.einsum('ptal,tbl->ptab', left_real, zero_imag) + jnp.einsum('ptal,tbl->ptab', left_imag, zero_real)
    offsets = (source_time[:, None] + jnp.arange(NT, dtype=jnp.int32)[None, :]) % NT
    selector = (offsets[:, :, None] == jnp.arange(NT, dtype=jnp.int32)[None, None, :]).astype(jnp.float32)
    result_real = jnp.einsum('adt,ptab->padb', selector, pair_real, precision=lax.Precision.HIGHEST)
    result_imag = jnp.einsum('adt,ptab->padb', selector, pair_imag, precision=lax.Precision.HIGHEST)
    return jnp.stack([result_real, result_imag], 1)
```

```python
import jax
import jax.numpy as jnp
import numpy as np
from jax import lax
from jax.experimental import pallas as pl
from jax.experimental.pallas import tpu as pltpu
from jax.sharding import PartitionSpec as P

SIDE = 48
NDIL = 4
LANES = 128
BF = jnp.bfloat16
F32 = jnp.float32


def mm(lhs, rhs, dims=((1,), (0,))):
    return lax.dot_general(lhs, rhs, (dims, ((), ())), preferred_element_type=F32)


def spread_matrix(vectors):
    k = np.arange(vectors)
    out = np.zeros((vectors, NDIL * LANES), np.float32)
    out[k, (k % NDIL) * LANES + k // NDIL] = 1
    return out


def owner_index(n_space, n_time, width):
    space, time, j = np.meshgrid(np.arange(n_space), np.arange(n_time), np.arange(width), indexing="ij")
    return ((time * n_space + space) * width + j).reshape(-1)


def pack_zero(real, imag):
    both = jnp.concatenate([real, imag], 0)
    third = both.shape[0] // 3
    return jnp.concatenate([both[i * third : (i + 1) * third] for i in range(3)], 1)


def unpack_zero(packed):
    both = jnp.concatenate([packed[:, i * LANES : (i + 1) * LANES] for i in range(3)], 0)
    half = both.shape[0] // 2
    return both[:half], both[half:]


def front_kernel(n_space, width, me_ref, sol_ref, eig_ref, dil_ref, spread_ref, turned_ref, zero_ref):
    columns = sol_ref.shape[-1]
    rows = columns // n_space
    me = me_ref[0]
    place = lax.broadcasted_iota(jnp.int32, (columns, LANES), 0).astype(F32) + 0.5
    rel = (place * (1.0 / rows)).astype(jnp.int32)
    inside = place - (rel * rows).astype(F32)
    time = (inside * (1.0 / width)).astype(jnp.int32)
    j = (inside - 0.5).astype(jnp.int32) - time * width
    dest = me + rel
    dest = jnp.where(dest >= n_space, dest - n_space, dest)
    target = (time * n_space + dest) * width + j
    lane = lax.broadcasted_iota(jnp.int32, (columns, LANES), 1)
    pick = jnp.concatenate(
        [jnp.where(target == lane + g * LANES, 1.0, 0.0) for g in range(columns // LANES)], 1
    ).astype(BF)
    turned = []
    for c in range(2):
        turned.append(mm(pick, sol_ref[c], ((1,), (1,))).astype(BF))
        turned_ref[c] = turned[c]
    pattern = mm(pick, dil_ref[...], ((1,), (1,)))
    vec_r = mm(eig_ref[0], spread_ref[...]).astype(BF)
    vec_i = mm(eig_ref[1], spread_ref[...]).astype(BF)
    real = mm(turned[0], vec_r) + mm(turned[1], vec_i)
    imag = mm(turned[1], vec_r) - mm(turned[0], vec_i)

    def masked(full):
        total = jnp.zeros((columns, LANES), F32)
        for d in range(NDIL):
            total = total + jnp.where(pattern == d, full[:, d * LANES : (d + 1) * LANES], 0.0)
        return total

    real, imag = masked(real), masked(imag)
    for r in range(n_space):
        to = me + r
        to = jnp.where(to >= n_space, to - n_space, to)
        zero_ref[to] = pack_zero(real[r * rows : (r + 1) * rows], imag[r * rows : (r + 1) * rows])


def momentum_kernel(rels, rows, turned_ref, eig_ref, cos_ref, sin_ref, *outs):
    moments = cos_ref.shape[0]
    spans = []
    for r in rels:
        if spans and spans[-1][1] == r:
            spans[-1][1] = r + 1
        else:
            spans.append([r, r + 1])
    ends = {r: i for i, r in enumerate(rels)}
    for first, last in spans:
        real_in = turned_ref[0, first * rows : last * rows].astype(F32)
        imag_in = turned_ref[1, first * rows : last * rows].astype(F32)
        for p in range(moments):
            cosine = cos_ref[p : p + 1]
            sine = sin_ref[p : p + 1]
            real = (cosine * real_in + sine * imag_in).astype(BF)
            imag = (cosine * imag_in - sine * real_in).astype(BF)
            out_r = mm(real, eig_ref[0]) + mm(imag, eig_ref[1])
            out_i = mm(imag, eig_ref[0]) - mm(real, eig_ref[1])
            half, at = divmod(p, moments // 2)
            for r in range(first, last):
                o = outs[2 * ends[r] + half]
                k = (r - first) * rows
                o[2 * at * rows : (2 * at + 1) * rows] = out_r[k : k + rows].astype(o.dtype)
                o[(2 * at + 1) * rows : (2 * at + 2) * rows] = out_i[k : k + rows].astype(o.dtype)


def back_kernel(
    n_space, hops, me_ref, *refs
):
    (z0, oa, ob, gbf, gbb, meson, undo, spread, order, dil) = refs[:10]
    fwd = refs[10 : 10 + hops]
    bwd = refs[10 + hops : 10 + 2 * hops - 1]
    out_ref, zr_ref, zi_ref = refs[10 + 2 * hops - 1 :]
    half = oa.shape[0]
    moments = meson.shape[0]
    rows = half // moments
    me = me_ref[0]
    total_a = oa[...] + fwd[-1][:half].astype(F32) + bwd[-1][:half].astype(F32)
    total_b = ob[...] + gbf[...].astype(F32) + gbb[...].astype(F32)
    coef = [total_a.astype(BF), total_b.astype(BF)]
    left, turned = [], []
    for p in range(moments):
        h, at = divmod(p, moments // 2)
        mine = coef[h][2 * at * rows : (2 * at + 2) * rows]
        by_r = mm(mine, meson[p, 0])
        by_i = mm(mine, meson[p, 1])
        left_r = (by_r[:rows] + by_i[rows:]).astype(BF)
        left_i = (by_i[:rows] - by_r[rows:]).astype(BF)
        left += [left_r, left_i]
    left = mm(jnp.concatenate(left, 0), spread[...]).astype(BF)
    for p in range(moments):
        turned += [-left[(2 * p + 1) * rows : (2 * p + 2) * rows], left[2 * p * rows : (2 * p + 1) * rows]]
    turned = jnp.concatenate(turned, 0)

    def put(packed, source):
        real, imag = unpack_zero(packed)
        start = pl.multiple_of(source * rows, rows)
        zr_ref[pl.ds(start, rows)] = real
        zi_ref[pl.ds(start, rows)] = imag

    put(z0[...], me)
    for r in range(hops):
        source = me - (r + 1)
        put(fwd[r][half:], jnp.where(source < 0, source + n_space, source))
    for r in range(hops - 1):
        source = me + (r + 1)
        put(bwd[r][half:], jnp.where(source >= n_space, source - n_space, source))
    pattern = dil[0:1]

    def expand(ref):
        natural = mm(ref[...], undo[...], ((0,), (0,)))
        return jnp.concatenate([jnp.where(pattern == d, natural, 0.0) for d in range(NDIL)], 0).astype(BF)

    pair = mm(left, expand(zr_ref)) + mm(turned, expand(zi_ref))
    out_ref[...] = mm(order[...], pair.astype(BF)).astype(BF)


def body(solutions, eigvecs, meson, momenta, source_time, dilution):
    times_local, _, colors, sites_local, columns = solutions.shape
    vectors = eigvecs.shape[4]
    moments = momenta.shape[0]
    n_space = lax.axis_size("space")
    n_time = lax.axis_size("tm")
    rows = columns // n_space
    width = rows // n_time
    hops = n_space // 2
    half = moments * rows
    me = lax.axis_index("space")
    me_arr = me.astype(jnp.int32).reshape(1)
    flat = colors * sites_local
    sol = solutions.reshape(2, flat, columns)
    eig = eigvecs.reshape(2, flat, vectors)

    site_index = me * sites_local + jnp.arange(sites_local, dtype=jnp.int32)
    coordinates = jnp.stack(
        [site_index % SIDE, site_index // SIDE % SIDE, site_index // (SIDE * SIDE)], 0
    )
    windings = jnp.sum(momenta[:, :, None] * coordinates[None], 1)
    angles = 2.0 * jnp.pi / SIDE * windings.astype(F32)
    cosine = jnp.tile(jnp.cos(angles), (1, colors))
    sine = jnp.tile(jnp.sin(angles), (1, colors))

    spread = jnp.asarray(spread_matrix(vectors), BF)
    natural = owner_index(n_space, n_time, width)
    undo = np.zeros((columns, columns), np.float32)
    undo[np.arange(columns), natural] = 1
    undo = jnp.asarray(undo, BF)
    place = np.arange(2 * half).reshape(moments * 2, n_time, width)
    order = np.zeros((2 * half, 2 * half), np.float32)
    order[np.arange(2 * half), np.swapaxes(place, 0, 1).reshape(-1)] = 1
    order = jnp.asarray(order, BF)
    dil_row = jnp.broadcast_to(dilution.astype(F32)[None], (LANES, columns))

    smem = pl.BlockSpec(memory_space=pltpu.SMEM)
    vmem = pl.BlockSpec(memory_space=pltpu.VMEM)
    packed = 2 * rows // 3

    def front(*args):
        return front_kernel(n_space, width, *args)

    turned, zero_parts = pl.pallas_call(
        front,
        out_shape=(
            jax.ShapeDtypeStruct((2, columns, flat), BF),
            jax.ShapeDtypeStruct((n_space, packed, 3 * LANES), F32),
        ),
        in_specs=[smem] + [vmem] * 4,
        out_specs=(vmem, vmem),
        name="front",
    )(me_arr, sol, eig, dil_row.astype(BF), spread)
    zero_all = lax.all_to_all(zero_parts, "space", split_axis=0, concat_axis=0, tiled=True)

    starts = ((hops, 0), (hops, 1), (hops - 1, 1), (hops + 1, 0))

    def momentum(rels, first):
        def run(*args):
            return momentum_kernel(rels, rows, *args)

        shapes = [
            jax.ShapeDtypeStruct((half, vectors), BF if (r, h) in starts else F32)
            for r in rels
            for h in range(2)
        ]
        outs = pl.pallas_call(
            run,
            out_shape=shapes,
            in_specs=[vmem] * 4,
            out_specs=[vmem] * len(shapes),
            name="momentum_first" if first else "momentum_rest",
        )(turned, eig, cosine, sine)
        return {r: (outs[2 * i], outs[2 * i + 1]) for i, r in enumerate(rels)}

    firsts = [hops - 1, hops, hops + 1]
    own = momentum(firsts, True)
    own.update(momentum([r for r in range(n_space) if r not in firsts], False))
    zero = jnp.sum(zero_all, 0).astype(BF)

    up = [(i, (i + 1) % n_space) for i in range(n_space)]
    down = [(i, (i - 1) % n_space) for i in range(n_space)]

    def at(r, h):
        return own[r % n_space][h]

    def grow(got, part):
        return (got.astype(F32) + part.astype(F32)).astype(BF)

    msg = {
        "bd": at(-hops, 1),
        "bu": at(hops - 1, 1),
        "au": jnp.concatenate([at(hops, 0), zero], 0),
        "ad": jnp.concatenate([at(1 - hops, 0), zero], 0),
    }
    left_to_go = {"bd": -hops, "bu": hops - 1, "au": hops, "ad": 1 - hops}
    got = {k: [] for k in msg}
    for step in range(hops):
        for k in ("bd", "au", "bu", "ad"):
            if len(got[k]) == abs(left_to_go[k]):
                continue
            distance = left_to_go[k]
            towards = 1 if distance > 0 else -1
            arrived = lax.ppermute(msg[k], "space", up if towards > 0 else down)
            got[k].append(arrived)
            following = distance - towards * len(got[k])
            if following != 0:
                h = 0 if k[0] == "a" else 1
                part = at(following, h)
                if h:
                    msg[k] = grow(arrived, part)
                else:
                    msg[k] = jnp.concatenate([grow(arrived[:half], part), arrived[half:]], 0)

    def back(*args):
        return back_kernel(n_space, hops, *args)

    operands = [
        zero, own[0][0], own[0][1], got["bu"][-1], got["bd"][-1],
        meson[:, 0], undo, spread, order, jnp.broadcast_to(dilution[None], (8, columns)),
        *got["au"], *got["ad"],
    ]
    outgoing = pl.pallas_call(
        back,
        out_shape=jax.ShapeDtypeStruct((2 * half, columns), BF),
        in_specs=[smem] + [vmem] * len(operands),
        out_specs=vmem,
        scratch_shapes=[pltpu.VMEM((columns, LANES), BF), pltpu.VMEM((columns, LANES), BF)],
        name="back",
    )(me_arr, *operands)

    wide = 2 * moments * width
    received = lax.all_to_all(
        outgoing.reshape(n_time, wide, columns), "tm", split_axis=0, concat_axis=0, tiled=True
    ).reshape(n_time * wide, columns)
    first_column = (lax.axis_index("tm") * n_space + me) * width
    sources = lax.dynamic_slice_in_dim(source_time, first_column, width)
    wanted = (sources[:, None] + jnp.arange(n_time, dtype=jnp.int32)[None]) % n_time
    wanted = jnp.broadcast_to(wanted[None], (2 * moments, width, n_time)).reshape(-1)
    lane_of = wanted * wide + jnp.arange(wide * n_time, dtype=jnp.int32) // n_time
    select = (lane_of[:, None] == jnp.arange(n_time * wide, dtype=jnp.int32)[None]).astype(BF)
    result = mm(select, received)
    return result.reshape(moments, 2, width, n_time, columns)


def solution(mesh):
    return jax.shard_map(
        body,
        mesh=mesh,
        in_specs=(
            P(("cfg", "tm"), None, None, "space", None),
            P(("cfg", "tm"), None, None, "space", None),
            P(None, ("cfg", "tm"), None, None, None),
            P(),
            P(),
            P(),
        ),
        out_specs=P(None, None, ("tm", "space"), "cfg", None),
        check_vma=False,
    )
```
